256 devices in a mesh: section: 4 (over y), dp: 64 (over x, z, core).
Axes of the slice: x: 4, y: 4, z: 8, core: 2. Of those that a mesh axis runs over, the one named last changes fastest.
Arguments:
- grads: float32 [4, 64, 512, 4096], P('section', 'dp'), may hold values from -8192 to 8192
- skipped: int32 [64], P('dp'), may hold values from 0 to 24
- master: float32 [4, 512, 4096], P('section', 'dp'), may hold values from -6 to 6
- moment_one: float32 [4, 512, 4096], P('section', 'dp'), may hold values from -6 to 6
- moment_two: float32 [4, 512, 4096], P('section', 'dp'), may hold values from 0.25 to 4
- bounds: int32 [4, 9], P('section'), may hold values from 0 to 512, as said below
- step: int32 [1], replicated, may hold values from 1 to 24
Outputs:
- params: bfloat16 [4, 512, 4096], P('section')
- master_next: float32 [4, 512, 4096], P('section', 'dp')
- moment_one_next: float32 [4, 512, 4096], P('section', 'dp')
- moment_two_next: float32 [4, 512, 4096], P('section', 'dp')
- layer_norms: float32 [4, 8], P('section')
- grad_norm: float32 [1], replicated
The draws below stay inside these ranges and needn't reach their ends.
Inputs may be any that keep to these rules, and one draw needn't show every extreme that they name: `bounds`: each section's row is strictly increasing, starts at 0 and ends at 512.
All inputs are finite; a program needn't handle non-finite values.
Results may differ from the reference program's by a relative error of at most 0.001.
Values may be sent and summed in bfloat16 or wider, within the bound.
No kernel may reach another device: no remote copies, remote signals or barrier semaphores. Data moves between devices by JAX's collectives and lax.ppermute only.
A program may use at most 64 MiB of HBM per device.

```python
import math
import jax
import jax.numpy as jnp
from jax import lax

D = 4096
LAYERS = 8
MICRO = 32
ROWS = 512
N_SECTION = 4
N_DP = 64


def section_bounds(key):
    inner = jax.random.permutation(key, ROWS - 1)[:LAYERS - 1] + 1
    inner = jnp.sort(inner.astype(jnp.int32))
    return jnp.concatenate([jnp.zeros((1,), jnp.int32), inner, jnp.full((1,), ROWS, jnp.int32)])


def draw_bounds(key, part):
    return jnp.stack([section_bounds(jax.random.fold_in(key, 7 + index)) for index in range(N_SECTION)])


def set_ends(drawn, stream_key, least, high):
    extent = drawn.shape
    spot = [jax.random.randint(jax.random.fold_in(stream_key, axis), (), 0, extent[axis]) for axis in range(len(extent))]
    drawn = drawn.at[tuple(spot)].set(least)
    longest = extent.index(max(extent))
    spot[longest] = (spot[longest] + 1) % extent[longest]
    return drawn.at[tuple(spot)].set(high)


def with_spikes(array, own_key, source, target, shards_of, factor):
    owner, partner = [(jnp.arange(array.shape[dim]) // (array.shape[dim] // shards_of)).reshape([-1 if axis == dim else 1 for axis in range(array.ndim)]) for dim in (source, target)]
    chosen = jax.random.permutation(own_key, shards_of)[partner]
    strong = (owner == chosen) | (owner == (partner + shards_of // 2) % shards_of)
    return jnp.where(strong, factor * array, array)


def shard_levels(key, shape, pieces, low, top_value):
    gain = 1.0
    for axis_at, blocks in pieces:
        heights = jax.random.uniform(jax.random.fold_in(jax.random.fold_in(key, 6), axis_at), (blocks,), jnp.float32, low / len(pieces), top_value / len(pieces))
        gain = gain * jnp.repeat(jnp.exp(heights), shape[axis_at] // blocks).reshape((-1,) + (1,) * (len(shape) - 1 - axis_at))
    return gain


def noise(rng, dims, width, bound, pieces=(), kind=jnp.bfloat16):
    drawn = jax.random.normal(rng, dims, jnp.float32) * width
    if len(pieces) > 0:
        drawn = shard_levels(rng, dims, pieces, -0.22, 0.18) * drawn
    return jnp.clip(drawn, min=-bound, max=bound).astype(kind)


def heavy_noise(rng, shape, scale, limit, cuts, heavy, held_as=jnp.bfloat16):
    values = scale * jax.random.normal(rng, shape, jnp.float32)
    if cuts:
        values = values * shard_levels(rng, shape, cuts, -0.22, 0.18)
    return jnp.clip(with_spikes(values, jax.random.fold_in(rng, 3), *heavy), -limit, limit).astype(held_as)


def setup_inputs(seed: int = 0) -> dict:
    seeds = jax.random.split(jax.random.key(seed), 8)
    return {
        "grads": heavy_noise(seeds[0], (N_SECTION, N_DP, ROWS, D), 500.0, 8192.0, ((0, 4), (1, 64)), (1, 2, 64, 4.0), jnp.float32),
        "skipped": set_ends(jax.random.randint(seeds[1], (N_DP,), 0, 25), jax.random.fold_in(seeds[1], 1), 0, 24).astype(jnp.int32),
        "master": noise(seeds[2], (N_SECTION, ROWS, D), 1.0, 6.0, ((0, 4), (1, 64)), jnp.float32),
        "moment_one": noise(seeds[3], (N_SECTION, ROWS, D), 1.0, 6.0, ((0, 4), (1, 64)), jnp.float32),
        "moment_two": jnp.clip(jnp.exp(math.log(4.0) - 2.7725887 * jax.random.uniform(seeds[4], (N_SECTION, ROWS, D), jnp.float32) ** shard_levels(seeds[4], (N_SECTION, ROWS, D), ((0, 4), (1, 64)), -0.2, 0.2)), 0.25, 4.0),
        "bounds": draw_bounds(jax.random.fold_in(seeds[7], 71), 0),
        "step": jax.random.randint(seeds[6], (1,), 1, 25).astype(jnp.int32),
    }


beta_one = 0.9
beta_two = 0.95
learn_rate = 0.05
weight_decay = 0.1
epsilon = 1e-08

def reference(grads, skipped, master, moment_one, moment_two, bounds, step):
    total_good = jnp.sum((MICRO - skipped).astype(jnp.float32))
    summed = lax.optimization_barrier(jnp.sum(grads, axis=1))
    mean_grad = summed / total_good
    row_squares = lax.optimization_barrier(jnp.sum(mean_grad * mean_grad, axis=2))
    row_index = jnp.arange(ROWS, dtype=jnp.int32)
    inside = (row_index[None, :, None] >= bounds[:, None, :-1]) & (row_index[None, :, None] < bounds[:, None, 1:])
    layer_sq = lax.optimization_barrier(jnp.sum(row_squares[:, :, None] * inside.astype(jnp.float32), axis=1))
    grad_rms = jnp.sqrt(jnp.sum(layer_sq) / (N_SECTION * ROWS * D))
    layer_rows = (bounds[:, 1:] - bounds[:, :-1]).astype(jnp.float32)
    layer_norms = jnp.sqrt(layer_sq / (layer_rows * D))
    clipped = mean_grad / jnp.maximum(1.0, grad_rms)
    first_next = beta_one * moment_one + (1.0 - beta_one) * clipped
    second_next = beta_two * moment_two + (1.0 - beta_two) * clipped * clipped
    step_value = step[0].astype(jnp.float32)
    fix_one = 1.0 - jnp.power(beta_one, step_value)
    fix_two = 1.0 - jnp.power(beta_two, step_value)
    update = first_next / fix_one / (jnp.sqrt(second_next / fix_two) + epsilon)
    master_next = master - learn_rate * (update + weight_decay * master)
    params = master_next.astype(jnp.bfloat16)
    return (params, master_next, first_next, second_next, layer_norms, grad_rms.reshape(1))
```

```python
import jax
import jax.numpy as jnp
from jax import lax
from jax.sharding import Mesh
from jax.sharding import PartitionSpec as P

MICRO = 32
DP = ("x", "z", "c")
ALL = ("section", "x", "z", "c")

beta_one = 0.9
beta_two = 0.95
learn_rate = 0.05
weight_decay = 0.1
epsilon = 1e-08

WIRE = jnp.float16
SCALE = 0.5


def swapped(value):
    return lax.ppermute(value, "c", [(0, 1), (1, 0)])


def exchanged(value, axis):
    return lax.all_to_all(value, axis, 0, 0, tiled=True)


def reduced_rows(flat, own_rows):
    n_x, n_z, n_c = (lax.axis_size(a) for a in DP)
    core = lax.axis_index("c")
    parts = flat.reshape(n_x, n_z, n_c, own_rows, flat.shape[1])
    kept = lax.dynamic_index_in_dim(parts, core, 2, keepdims=False) * SCALE
    sent = lax.dynamic_index_in_dim(parts, 1 - core, 2, keepdims=False) * SCALE
    chip = kept + swapped(sent.astype(WIRE)).astype(jnp.float32)
    along_x = exchanged(chip.astype(WIRE), "x").astype(jnp.float32).sum(axis=0)
    along_z = exchanged(along_x.astype(WIRE), "z").astype(jnp.float32).sum(axis=0)
    return along_z * (1.0 / SCALE)


def gathered_rows(rows):
    n_x, n_z, n_c = (lax.axis_size(a) for a in DP)
    core = lax.axis_index("c")
    along_z = exchanged(jnp.broadcast_to(rows[None], (n_z, *rows.shape)), "z")
    along_x = exchanged(jnp.broadcast_to(along_z[None], (n_x, *along_z.shape)), "x")
    other = swapped(along_x)
    first = core == 0
    both = jnp.stack(
        [jnp.where(first, along_x, other), jnp.where(first, other, along_x)], axis=2
    )
    return both.reshape(n_x * n_z * n_c * rows.shape[0], rows.shape[1])


def on_device(grads, skipped, master, moment_one, moment_two, bounds, step):
    flat_grads = grads[0, 0]
    rows_all, width = flat_grads.shape
    own_rows = master.shape[1]
    layers = bounds.shape[1] - 1
    n_section = lax.axis_size("section")
    n_all = lax.axis_size(ALL)
    summed = reduced_rows(flat_grads, own_rows)

    row_index = lax.axis_index(DP) * own_rows + jnp.arange(own_rows, dtype=jnp.int32)
    inside = (row_index[:, None] >= bounds[0, None, :-1]) & (
        row_index[:, None] < bounds[0, None, 1:]
    )
    row_squares = jnp.sum(summed * summed, axis=1)
    layer_part = jnp.sum(row_squares[:, None] * inside.astype(jnp.float32), axis=0)
    good = (MICRO - skipped).astype(jnp.float32)
    report = jnp.concatenate([layer_part, good])
    reports = exchanged(jnp.broadcast_to(report[None], (n_all, layers + 1)), ALL)
    sections = reports.reshape(n_section, -1, layers + 1).sum(axis=1)
    total_good = sections[0, layers]
    squares = sections[:, :layers] / (total_good * total_good)
    layer_sq = lax.dynamic_index_in_dim(
        squares, lax.axis_index("section"), 0, keepdims=False
    )
    grad_rms = jnp.sqrt(jnp.sum(squares) / (n_section * rows_all * width))
    layer_rows = (bounds[0, 1:] - bounds[0, :-1]).astype(jnp.float32)
    layer_norms = jnp.sqrt(layer_sq / (layer_rows * width))

    clipped = summed / total_good / jnp.maximum(1.0, grad_rms)
    first_next = beta_one * moment_one[0] + (1.0 - beta_one) * clipped
    second_next = beta_two * moment_two[0] + (1.0 - beta_two) * clipped * clipped
    step_value = step[0].astype(jnp.float32)
    fix_one = 1.0 - jnp.power(beta_one, step_value)
    fix_two = 1.0 - jnp.power(beta_two, step_value)
    update = first_next / fix_one / (jnp.sqrt(second_next / fix_two) + epsilon)
    master_next = master[0] - learn_rate * (update + weight_decay * master[0])
    gathered = gathered_rows(master_next.astype(jnp.bfloat16))
    return (
        gathered[None],
        master_next[None],
        first_next[None],
        second_next[None],
        layer_norms[None],
        grad_rms.reshape(1),
    )


def solution(mesh):
    split = Mesh(
        mesh.devices.reshape(mesh.shape["section"], 4, 8, 2), ("section", "x", "z", "c")
    )
    placed = (
        P("section", DP, None, None),
        P(DP),
        P("section", DP, None),
        P("section", DP, None),
        P("section", DP, None),
        P("section", None),
        P(),
    )
    return jax.shard_map(
        on_device,
        mesh=split,
        in_specs=placed,
        out_specs=(
            P("section", None, None),
            P("section", DP, None),
            P("section", DP, None),
            P("section", DP, None),
            P("section", None),
            P(),
        ),
        check_vma=False,
    )
```

```python
import jax
import jax.numpy as jnp
from jax import lax
from jax.experimental import pallas as pl
from jax.experimental.pallas import tpu as pltpu
from jax.sharding import Mesh
from jax.sharding import PartitionSpec as P


MICRO = 32
DP = ("x", "z", "c")
ALL = ("section", "x", "z", "c")

beta_one = 0.9
beta_two = 0.95
learn_rate = 0.05
weight_decay = 0.1
epsilon = 1e-08

WIRE = jnp.float16
SCALE = 0.5

SUM_SHARE = 7
GATHER_SHARE = 6


def swapped(value):
    return lax.ppermute(value, "c", [(0, 1), (1, 0)])


def shifted(value, axis, k):
    n = lax.axis_size(axis)
    return lax.ppermute(value, axis, [(i, (i + k) % n) for i in range(n)])


def exchanged(value, axis):
    return lax.all_to_all(value, axis, 0, 0, tiled=True)


def hops(n):
    return sorted(range(1, n), key=lambda k: -min(k, n - k))


def piece(parts, at_x, core, first, width):
    n_x, n_z, _, rows, _ = parts.shape
    start = (0 if at_x is None else at_x, 0, core, 0, first)
    taken = (n_x if at_x is None else 1, n_z, 1, rows, width)
    return lax.dynamic_slice(parts, start, taken)[:, :, 0] * SCALE


def at(values, i):
    return lax.dynamic_index_in_dim(values, i, 0, keepdims=False).astype(jnp.float32)


def reduced_rows(flat, own_rows):
    n_x, n_z, n_c = (lax.axis_size(a) for a in DP)
    x, core = lax.axis_index("x"), lax.axis_index("c")
    width = flat.shape[1]
    parts = flat.reshape(n_x, n_z, n_c, own_rows, width)
    wide = width * SUM_SHARE // 8

    def chip_a(k):
        to_x = (x + k) % n_x
        sent = piece(parts, to_x, 1 - core, 0, wide)[0].astype(WIRE)
        return piece(parts, to_x, core, 0, wide)[0] + swapped(sent).astype(jnp.float32)

    arrived = [shifted(chip_a(k).astype(WIRE), "x", k) for k in hops(n_x)]
    a_x = chip_a(0)
    sent = piece(parts, None, 1 - core, wide, width - wide).astype(WIRE)
    chip_b = piece(parts, None, core, wide, width - wide)
    chip_b = chip_b + swapped(sent).astype(jnp.float32)
    b_z = exchanged(chip_b.astype(WIRE).transpose(1, 0, 2, 3), "z")
    b_z = b_z.astype(jnp.float32).sum(axis=0)
    for value in arrived:
        a_x = a_x + value.astype(jnp.float32)
    b_sent = [shifted(at(b_z, (x + k) % n_x).astype(WIRE), "x", k) for k in hops(n_x)]
    a_z = exchanged(a_x.astype(WIRE), "z").astype(jnp.float32).sum(axis=0)
    b_x = at(b_z, x)
    for value in b_sent:
        b_x = b_x + value.astype(jnp.float32)
    return jnp.concatenate([a_z, b_x], axis=1) * (1.0 / SCALE)


def placed_rows(slots, a_parts, b_part, out=None):
    n_x = len(a_parts)
    n_z, rows, wide = a_parts[0].shape
    narrow = b_part.shape[-1]

    def kernel(*refs):
        slots, a_in, b_in = refs[0], refs[1 : 1 + n_x], refs[1 + n_x]
        to, sems = refs[-2:]
        copies = []
        for j in range(n_x):
            there = to.at[slots[1 + j], :, slots[0]]
            copies.append((a_in[j], there.at[:, :, pl.ds(0, wide)]))
            copies.append((b_in.at[:, j], there.at[:, :, pl.ds(wide, narrow)]))
        copies = [
            pltpu.make_async_copy(*pair, sems.at[i]) for i, pair in enumerate(copies)
        ]
        for copy in copies:
            copy.start()
        for copy in copies:
            copy.wait()

    near = pl.BlockSpec(memory_space=pltpu.VMEM)
    far = pl.BlockSpec(memory_space=pltpu.HBM)
    operands = [slots, *a_parts, b_part] + ([] if out is None else [out])
    specs = [pl.BlockSpec(memory_space=pltpu.SMEM)] + [near] * (n_x + 1)
    return pl.pallas_call(
        kernel,
        out_shape=jax.ShapeDtypeStruct(
            (n_x, n_z, 2, rows, wide + narrow), a_parts[0].dtype
        ),
        in_specs=specs + [far] * (len(operands) - len(specs)),
        out_specs=far,
        scratch_shapes=[pltpu.SemaphoreType.DMA((2 * n_x,))],
        input_output_aliases={} if out is None else {len(operands) - 1: 0},
        compiler_params=pltpu.CompilerParams(vmem_limit_bytes=8 << 20),
    )(*operands)


def gathered_rows(rows):
    n_x, n_z, n_c = (lax.axis_size(a) for a in DP)
    x, core = lax.axis_index("x"), lax.axis_index("c")
    own_rows, width = rows.shape
    wide = width * GATHER_SHARE // 8
    shifts = [0] + hops(n_x)
    a, b = rows[:, :wide], rows[:, wide:]
    b_x = jnp.stack([b] + [shifted(b, "x", k) for k in shifts[1:]])
    a_z = exchanged(jnp.broadcast_to(a[None], (n_z, *a.shape)), "z")
    a_all = [a_z] + [shifted(a_z, "x", k) for k in shifts[1:]]
    b_all = exchanged(jnp.broadcast_to(b_x[None], (n_z, *b_x.shape)), "z")
    a_other = [swapped(v) for v in a_all]
    b_other = swapped(b_all)
    origins = [lax.rem(x + (n_x - k), n_x) for k in shifts]
    out = placed_rows(jnp.stack([core] + origins), a_all, b_all)
    out = placed_rows(jnp.stack([1 - core] + origins), a_other, b_other, out)
    return out.reshape(n_x * n_z * n_c * own_rows, width)


def on_device(grads, skipped, master, moment_one, moment_two, bounds, step):
    flat_grads = grads[0, 0]
    rows_all, width = flat_grads.shape
    own_rows = master.shape[1]
    layers = bounds.shape[1] - 1
    n_section = lax.axis_size("section")
    n_all = lax.axis_size(ALL)
    summed = reduced_rows(flat_grads, own_rows)

    row_index = lax.axis_index(DP) * own_rows + jnp.arange(own_rows, dtype=jnp.int32)
    inside = (row_index[:, None] >= bounds[0, None, :-1]) & (
        row_index[:, None] < bounds[0, None, 1:]
    )
    row_squares = jnp.sum(summed * summed, axis=1)
    layer_part = jnp.sum(row_squares[:, None] * inside.astype(jnp.float32), axis=0)
    good = (MICRO - skipped).astype(jnp.float32)
    report = jnp.concatenate([layer_part, good])
    reports = exchanged(jnp.broadcast_to(report[None], (n_all, layers + 1)), ALL)
    sections = reports.reshape(n_section, -1, layers + 1).sum(axis=1)
    total_good = sections[0, layers]
    squares = sections[:, :layers] / (total_good * total_good)
    layer_sq = lax.dynamic_index_in_dim(
        squares, lax.axis_index("section"), 0, keepdims=False
    )
    grad_rms = jnp.sqrt(jnp.sum(squares) / (n_section * rows_all * width))
    layer_rows = (bounds[0, 1:] - bounds[0, :-1]).astype(jnp.float32)
    layer_norms = jnp.sqrt(layer_sq / (layer_rows * width))

    clipped = summed / total_good / jnp.maximum(1.0, grad_rms)
    first_next = beta_one * moment_one[0] + (1.0 - beta_one) * clipped
    second_next = beta_two * moment_two[0] + (1.0 - beta_two) * clipped * clipped
    step_value = step[0].astype(jnp.float32)
    fix_one = 1.0 - jnp.power(beta_one, step_value)
    fix_two = 1.0 - jnp.power(beta_two, step_value)
    update = first_next / fix_one / (jnp.sqrt(second_next / fix_two) + epsilon)
    master_next = master[0] - learn_rate * (update + weight_decay * master[0])
    gathered = gathered_rows(master_next.astype(jnp.bfloat16))
    return (
        gathered[None],
        master_next[None],
        first_next[None],
        second_next[None],
        layer_norms[None],
        grad_rms.reshape(1),
    )


def solution(mesh):
    split = Mesh(
        mesh.devices.reshape(mesh.shape["section"], 4, 8, 2), ("section", "x", "z", "c")
    )
    placed = (
        P("section", DP, None, None),
        P(DP),
        P("section", DP, None),
        P("section", DP, None),
        P("section", DP, None),
        P("section", None),
        P(),
    )

    return jax.shard_map(
        on_device,
        mesh=split,
        in_specs=placed,
        out_specs=(
            P("section", None, None),
            P("section", DP, None),
            P("section", DP, None),
            P("section", DP, None),
            P("section", None),
            P(),
        ),
        check_vma=False,
    )
```

```python
import jax
import jax.numpy as jnp
from jax import lax
from jax.experimental import pallas as pl
from jax.experimental.pallas import tpu as pltpu
from jax.sharding import Mesh
from jax.sharding import PartitionSpec as P


MICRO = 32
DP = ("x", "z", "c")
ALL = ("section", "x", "z", "c")

beta_one = 0.9
beta_two = 0.95
learn_rate = 0.05
weight_decay = 0.1
epsilon = 1e-08

WIRE = jnp.float16
SCALE = 0.5

SUM_SHARE = 14
GATHER_SHARE = 13


def swapped(value):
    return lax.ppermute(value, "c", [(0, 1), (1, 0)])


def shifted(value, axis, k):
    n = lax.axis_size(axis)
    return lax.ppermute(value, axis, [(i, (i + k) % n) for i in range(n)])


def exchanged(value, axis):
    return lax.all_to_all(value, axis, 0, 0, tiled=True)


def hops(n):
    return sorted(range(1, n), key=lambda k: -min(k, n - k))


def piece(parts, at_x, core, first, width):
    n_x, n_z, _, rows, _ = parts.shape
    start = (0 if at_x is None else at_x, 0, core, 0, first)
    taken = (n_x if at_x is None else 1, n_z, 1, rows, width)
    return lax.dynamic_slice(parts, start, taken)[:, :, 0] * SCALE


def at(values, i):
    return lax.dynamic_index_in_dim(values, i, 0, keepdims=False).astype(jnp.float32)


def after(value, *others):
    return lax.optimization_barrier((value, *others))[0]


def reduced_rows(flat, own_rows):
    n_x, n_z, n_c = (lax.axis_size(a) for a in DP)
    x, core = lax.axis_index("x"), lax.axis_index("c")
    width = flat.shape[1]
    parts = flat.reshape(n_x, n_z, n_c, own_rows, width)
    wide = width * SUM_SHARE // 16

    def encoded(source, k):
        return piece(source, (x + k) % n_x, 1 - core, 0, wide)[0].astype(WIRE)

    def summed_chip(source, k, other):
        return piece(source, (x + k) % n_x, core, 0, wide)[0] + other.astype(jnp.float32)

    order = hops(n_x)
    sent = [encoded(parts, k) for k in order]
    sent_b = piece(after(parts, *sent), None, 1 - core, wide, width - wide).astype(WIRE)
    other = [swapped(v) for v in sent]
    other_b = swapped(sent_b)
    chips = [
        summed_chip(parts, k, v).astype(WIRE) for k, v in zip(order, other, strict=True)
    ]
    arrived = [shifted(v, "x", k) for k, v in zip(order, chips, strict=True)]
    late = after(parts, *chips)
    chip_b = piece(late, None, core, wide, width - wide)
    chip_b = chip_b + other_b.astype(jnp.float32)
    chip_b = chip_b.transpose(1, 0, 2, 3).astype(WIRE)
    b_z = exchanged(chip_b, "z")
    b_z = b_z.astype(jnp.float32).sum(axis=0)
    late = after(parts, chip_b)
    own = encoded(late, 0)
    own = swapped(own)
    a_x = lax.optimization_barrier(summed_chip(late, 0, own))
    for value in arrived:
        a_x = a_x + value.astype(jnp.float32)
    b_sent = [shifted(at(b_z, (x + k) % n_x).astype(WIRE), "x", k) for k in hops(n_x)]
    a_z = exchanged(a_x.astype(WIRE), "z").astype(jnp.float32).sum(axis=0)
    b_x = at(b_z, x)
    for value in b_sent:
        b_x = b_x + value.astype(jnp.float32)
    return jnp.concatenate([a_z, b_x], axis=1) * (1.0 / SCALE)


def stepped(summed, good, clip, moment_one, moment_two, master, fix_one, fix_two):
    clipped = summed / good / clip
    first_next = beta_one * moment_one + (1.0 - beta_one) * clipped
    second_next = beta_two * moment_two + (1.0 - beta_two) * clipped * clipped
    update = first_next / fix_one / (jnp.sqrt(second_next / fix_two) + epsilon)
    master_next = master - learn_rate * (update + weight_decay * master)
    return master_next, first_next, second_next


def normed_rows(reports, summed, moment_one, moment_two, master, section, fixes, sizes):
    n_section, n_z, wide, elements = sizes
    rows, width = summed.shape
    columns = reports.shape[-1]
    each = reports.shape[0] // n_section

    def kernel(section, fixes, reports, summed, one, two, master, a, b, facts):
        sums = [
            jnp.sum(reports[pl.ds(i * each, each)], axis=0) for i in range(n_section)
        ]
        good = sums[0][:, columns - 1 :]
        squares = [v / (good * good) for v in sums]
        own, total = squares[0], squares[0]
        for i in range(1, n_section):
            own = jnp.where(section[0] == i, squares[i], own)
            total = total + squares[i]
        lane = lax.broadcasted_iota(jnp.int32, total.shape, 1)
        total = jnp.where(lane < columns - 1, total, 0.0)
        norm = jnp.sqrt(jnp.sum(total, axis=1, keepdims=True) / elements)
        clip = jnp.maximum(1.0, norm)
        facts[0:1] = own
        for i, value in enumerate((good, clip, norm)):
            facts[i + 1 : i + 2] = jnp.broadcast_to(value, own.shape)
        master_next = stepped(
            summed[...], good, clip, one[...], two[...], master[...], fixes[0], fixes[1]
        )[0]
        sent = master_next.astype(a.dtype)
        a[...] = jnp.broadcast_to(sent[None, :, :wide], a.shape)
        b[...] = sent[:, wide:]

    scalar = pl.BlockSpec(memory_space=pltpu.SMEM)
    near = pl.BlockSpec(memory_space=pltpu.VMEM)
    return pl.pallas_call(
        kernel,
        out_shape=(
            jax.ShapeDtypeStruct((n_z, rows, wide), jnp.bfloat16),
            jax.ShapeDtypeStruct((rows, width - wide), jnp.bfloat16),
            jax.ShapeDtypeStruct((4, columns), jnp.float32),
        ),
        in_specs=[scalar] * 2 + [near] * 5,
        out_specs=(near, near, near),
        compiler_params=pltpu.CompilerParams(vmem_limit_bytes=8 << 20),
    )(section, fixes, reports, summed, moment_one, moment_two, master)


def placed_rows(shape, spots, pieces, out=None):
    total = sum(1 if axis is None else v.shape[axis] for v, axis, _ in pieces)

    def kernel(*refs):
        spots, ins, to, sems = refs[0], refs[1 : 1 + len(pieces)], refs[-2], refs[-1]
        copies = []
        for ref, (_, axis, first) in zip(ins, pieces, strict=True):
            views = [ref]
            if axis is not None:
                views = [ref.at[:, j] for j in range(ref.shape[axis])]
            for view in views:
                i = len(copies)
                columns = pl.ds(first, view.shape[-1])
                there = to.at[spots[2 * i], :, spots[2 * i + 1], :, columns]
                copies.append(pltpu.make_async_copy(view, there, sems.at[i]))
        for copy in copies:
            copy.start()
        for copy in copies:
            copy.wait()

    near = pl.BlockSpec(memory_space=pltpu.VMEM)
    far = pl.BlockSpec(memory_space=pltpu.HBM)
    operands = [spots, *(v for v, _, _ in pieces)] + ([] if out is None else [out])
    specs = [pl.BlockSpec(memory_space=pltpu.SMEM)] + [near] * len(pieces)
    return pl.pallas_call(
        kernel,
        out_shape=jax.ShapeDtypeStruct(shape, pieces[0][0].dtype),
        in_specs=specs + [far] * (len(operands) - len(specs)),
        out_specs=far,
        scratch_shapes=[pltpu.SemaphoreType.DMA((total,))],
        input_output_aliases={} if out is None else {len(operands) - 1: 0},
        compiler_params=pltpu.CompilerParams(vmem_limit_bytes=8 << 20),
    )(*operands)


def gathered_rows(a, b):
    n_x, n_z, n_c = (lax.axis_size(a) for a in DP)
    x, core = lax.axis_index("x"), lax.axis_index("c")
    own_rows, width = b.shape[0], a.shape[2] + b.shape[1]
    shifts = [0] + hops(n_x)
    b_x = [b] + [shifted(b, "x", k) for k in shifts[1:]]
    b_x = jnp.stack(b_x)
    b_x = jnp.broadcast_to(b_x[None], (n_z, *b_x.shape))
    a_z = exchanged(a, "z")
    a_all = [a_z, shifted(a_z, "x", shifts[1])]
    a_all += [shifted(a_z, "x", k) for k in shifts[2:]]
    b_all = exchanged(b_x, "z")
    a_other = [swapped(v) for v in a_all]
    b_other = swapped(b_all)
    origin = [lax.rem(x + (n_x - k), n_x) for k in shifts]
    wide = a.shape[2]
    shape = (n_x, n_z, n_c, own_rows, width)

    def spots(*pairs):
        return jnp.stack([v for pair in pairs for v in pair])

    out = placed_rows(
        shape,
        spots(*((origin[j], c) for j in (0, 1) for c in (core, 1 - core))),
        [(v[j], None, 0) for j in (0, 1) for v in (a_all, a_other)],
    )
    for a_last, b_last, c in ((a_all, b_all, core), (a_other, b_other, 1 - core)):
        out = placed_rows(
            shape,
            spots(*((origin[j], c) for j in range(2, n_x)), *((o, c) for o in origin)),
            [(v, None, 0) for v in a_last[2:]] + [(b_last, 1, wide)],
            out,
        )
    return out.reshape(n_x * n_z * n_c * own_rows, width)


def on_device(grads, skipped, master, moment_one, moment_two, bounds, step):
    flat_grads = grads[0, 0]
    rows_all, width = flat_grads.shape
    own_rows = master.shape[1]
    layers = bounds.shape[1] - 1
    n_section = lax.axis_size("section")
    n_all = lax.axis_size(ALL)
    summed = reduced_rows(flat_grads, own_rows)

    row_index = lax.axis_index(DP) * own_rows + jnp.arange(own_rows, dtype=jnp.int32)
    inside = (row_index[:, None] >= bounds[0, None, :-1]) & (
        row_index[:, None] < bounds[0, None, 1:]
    )
    row_squares = jnp.sum(summed * summed, axis=1)
    layer_part = jnp.sum(row_squares[:, None] * inside.astype(jnp.float32), axis=0)
    good = (MICRO - skipped).astype(jnp.float32)
    report = jnp.concatenate([layer_part, good])
    reports = exchanged(jnp.broadcast_to(report, (n_all, 1, layers + 1)), ALL)
    step_value = step[0].astype(jnp.float32)
    fix_one = 1.0 - jnp.power(beta_one, step_value)
    fix_two = 1.0 - jnp.power(beta_two, step_value)
    state = (moment_one[0], moment_two[0], master[0])
    sizes = (
        n_section,
        lax.axis_size("z"),
        width * GATHER_SHARE // 16,
        n_section * rows_all * width,
    )
    a, b, facts = normed_rows(
        reports,
        summed,
        *state,
        lax.axis_index("section").reshape(1),
        jnp.stack([fix_one, fix_two]),
        sizes,
    )
    gathered = gathered_rows(a, b)
    good, clip, grad_rms = facts[1, 0], facts[2, 0], facts[3, 0]
    layer_rows = (bounds[0, 1:] - bounds[0, :-1]).astype(jnp.float32)
    layer_norms = jnp.sqrt(facts[0, :layers] / (layer_rows * width))
    master_next, first_next, second_next = stepped(
        summed, good, clip, *state, fix_one, fix_two
    )
    return (
        gathered[None],
        master_next[None],
        first_next[None],
        second_next[None],
        layer_norms[None],
        grad_rms.reshape(1),
    )


def solution(mesh):
    split = Mesh(
        mesh.devices.reshape(mesh.shape["section"], 4, 8, 2), ("section", "x", "z", "c")
    )
    placed = (
        P("section", DP, None, None),
        P(DP),
        P("section", DP, None),
        P("section", DP, None),
        P("section", DP, None),
        P("section", None),
        P(),
    )

    return jax.shard_map(
        on_device,
        mesh=split,
        in_specs=placed,
        out_specs=(
            P("section", None, None),
            P("section", DP, None),
            P("section", DP, None),
            P("section", DP, None),
            P("section", None),
            P(),
        ),
        check_vma=False,
    )
```

```python
import jax
import jax.numpy as jnp
from jax import lax
from jax.experimental import pallas as pl
from jax.experimental.pallas import tpu as pltpu
from jax.sharding import Mesh
from jax.sharding import PartitionSpec as P


MICRO = 32
DP = ("x", "z", "c")
ALL = ("section", "x", "z", "c")

beta_one = 0.9
beta_two = 0.95
learn_rate = 0.05
weight_decay = 0.1
epsilon = 1e-08

WIRE = jnp.float16
SCALE = 0.25

SUM_SHARE = 14
GATHER_SHARE = 13


def swapped(value):
    return lax.ppermute(value, "c", [(0, 1), (1, 0)])


def shifted(value, axis, k):
    n = lax.axis_size(axis)
    return lax.ppermute(value, axis, [(i, (i + k) % n) for i in range(n)])


def exchanged(value, axis):
    return lax.all_to_all(value, axis, 0, 0, tiled=True)


def hops(n):
    return sorted(range(1, n), key=lambda k: -min(k, n - k))


def piece(parts, at_x, core, first, width):
    n_x, n_z, _, rows, _ = parts.shape
    start = (0 if at_x is None else at_x, 0, core, 0, first)
    taken = (n_x if at_x is None else 1, n_z, 1, rows, width)
    return lax.dynamic_slice(parts, start, taken)[:, :, 0] * SCALE


def at(values, i):
    return lax.dynamic_index_in_dim(values, i, 0, keepdims=False).astype(jnp.float32)


def after(value, *others):
    return lax.optimization_barrier((value, *others))[0]


def reduced_rows(flat, own_rows):
    n_x, n_z, n_c = (lax.axis_size(a) for a in DP)
    x, core = lax.axis_index("x"), lax.axis_index("c")
    width = flat.shape[1]
    parts = flat.reshape(n_x, n_z, n_c, own_rows, width)
    wide = width * SUM_SHARE // 16

    def encoded(source, k):
        return piece(source, (x + k) % n_x, 1 - core, 0, wide)[0].astype(WIRE)

    def summed_chip(source, k, other):
        return piece(source, (x + k) % n_x, core, 0, wide)[0] + other.astype(jnp.float32)

    far, *near = hops(n_x)
    far_sent = encoded(parts, far)
    near_sent = [encoded(after(parts, far_sent), k) for k in near]
    far_other = swapped(far_sent)
    near_other = [swapped(v) for v in near_sent]
    far_chip = summed_chip(parts, far, far_other).astype(WIRE)
    far_in = shifted(far_chip, "x", far)
    late = after(parts, far_chip)
    chips = [
        summed_chip(late, k, v).astype(WIRE)
        for k, v in zip(near, near_other, strict=True)
    ]
    near_in = [shifted(v, "x", k) for k, v in zip(near, chips, strict=True)]
    late = after(parts, *chips)
    sent_b = piece(late, None, 1 - core, wide, width - wide).astype(WIRE)
    other_b = swapped(sent_b)
    late = after(parts, sent_b)
    chip_b = piece(late, None, core, wide, width - wide)
    chip_b = chip_b + other_b.astype(jnp.float32)
    chip_b = chip_b.transpose(1, 0, 2, 3).astype(WIRE)
    b_z = exchanged(chip_b, "z")
    b_z = b_z.astype(jnp.float32).sum(axis=0)
    late = after(parts, chip_b)
    own = encoded(late, 0)
    own = swapped(own)
    a_x = summed_chip(late, 0, own) + far_in.astype(jnp.float32)
    a_x = lax.optimization_barrier(a_x)
    for value in near_in:
        a_x = a_x + value.astype(jnp.float32)
    b_sent = [shifted(at(b_z, (x + k) % n_x).astype(WIRE), "x", k) for k in hops(n_x)]
    a_z = exchanged(a_x.astype(WIRE), "z").astype(jnp.float32).sum(axis=0)
    b_x = at(b_z, x)
    for value in b_sent:
        b_x = b_x + value.astype(jnp.float32)
    return jnp.concatenate([a_z, b_x], axis=1) * (1.0 / SCALE)


def stepped(summed, good, clip, moment_one, moment_two, master, fix_one, fix_two):
    clipped = summed / good / clip
    first_next = beta_one * moment_one + (1.0 - beta_one) * clipped
    second_next = beta_two * moment_two + (1.0 - beta_two) * clipped * clipped
    update = first_next / fix_one / (jnp.sqrt(second_next / fix_two) + epsilon)
    master_next = master - learn_rate * (update + weight_decay * master)
    return master_next, first_next, second_next


def normed_rows(reports, summed, moment_one, moment_two, master, section, fixes, sizes):
    n_section, n_z, wide, elements = sizes
    rows, width = summed.shape
    columns = reports.shape[-1]
    each = reports.shape[0] // n_section

    def kernel(section, fixes, reports, summed, one, two, master, a, b, facts):
        sums = [
            jnp.sum(reports[pl.ds(i * each, each)], axis=0) for i in range(n_section)
        ]
        good = sums[0][:, columns - 1 :]
        squares = [v / (good * good) for v in sums]
        own, total = squares[0], squares[0]
        for i in range(1, n_section):
            own = jnp.where(section[0] == i, squares[i], own)
            total = total + squares[i]
        lane = lax.broadcasted_iota(jnp.int32, total.shape, 1)
        total = jnp.where(lane < columns - 1, total, 0.0)
        norm = jnp.sqrt(jnp.sum(total, axis=1, keepdims=True) / elements)
        clip = jnp.maximum(1.0, norm)
        facts[0:1] = own
        for i, value in enumerate((good, clip, norm)):
            facts[i + 1 : i + 2] = jnp.broadcast_to(value, own.shape)
        master_next = stepped(
            summed[...], good, clip, one[...], two[...], master[...], fixes[0], fixes[1]
        )[0]
        sent = master_next.astype(a.dtype)
        a[...] = jnp.broadcast_to(sent[None, :, :wide], a.shape)
        b[...] = sent[:, wide:]

    scalar = pl.BlockSpec(memory_space=pltpu.SMEM)
    near = pl.BlockSpec(memory_space=pltpu.VMEM)
    return pl.pallas_call(
        kernel,
        out_shape=(
            jax.ShapeDtypeStruct((n_z, rows, wide), jnp.bfloat16),
            jax.ShapeDtypeStruct((rows, width - wide), jnp.bfloat16),
            jax.ShapeDtypeStruct((4, columns), jnp.float32),
        ),
        in_specs=[scalar] * 2 + [near] * 5,
        out_specs=(near, near, near),
        compiler_params=pltpu.CompilerParams(vmem_limit_bytes=8 << 20),
    )(section, fixes, reports, summed, moment_one, moment_two, master)


def placed_rows(shape, spots, pieces, out=None):
    total = sum(1 if axis is None else v.shape[axis] for v, axis, _ in pieces)

    def kernel(*refs):
        spots, ins, to, sems = refs[0], refs[1 : 1 + len(pieces)], refs[-2], refs[-1]
        copies = []
        for ref, (_, axis, first) in zip(ins, pieces, strict=True):
            views = [ref]
            if axis is not None:
                views = [ref.at[:, j] for j in range(ref.shape[axis])]
            for view in views:
                i = len(copies)
                columns = pl.ds(first, view.shape[-1])
                there = to.at[spots[2 * i], :, spots[2 * i + 1], :, columns]
                copies.append(pltpu.make_async_copy(view, there, sems.at[i]))
        for copy in copies:
            copy.start()
        for copy in copies:
            copy.wait()

    near = pl.BlockSpec(memory_space=pltpu.VMEM)
    far = pl.BlockSpec(memory_space=pltpu.HBM)
    operands = [spots, *(v for v, _, _ in pieces)] + ([] if out is None else [out])
    specs = [pl.BlockSpec(memory_space=pltpu.SMEM)] + [near] * len(pieces)
    return pl.pallas_call(
        kernel,
        out_shape=jax.ShapeDtypeStruct(shape, pieces[0][0].dtype),
        in_specs=specs + [far] * (len(operands) - len(specs)),
        out_specs=far,
        scratch_shapes=[pltpu.SemaphoreType.DMA((total,))],
        input_output_aliases={} if out is None else {len(operands) - 1: 0},
        compiler_params=pltpu.CompilerParams(vmem_limit_bytes=8 << 20),
    )(*operands)


def gathered_rows(a, b):
    n_x, n_z, n_c = (lax.axis_size(a) for a in DP)
    x, core = lax.axis_index("x"), lax.axis_index("c")
    own_rows, width = b.shape[0], a.shape[2] + b.shape[1]
    shifts = [0] + hops(n_x)
    b_x = [b] + [shifted(b, "x", k) for k in shifts[1:]]
    b_x = jnp.stack(b_x)
    b_x = jnp.broadcast_to(b_x[None], (n_z, *b_x.shape))
    a_z = exchanged(a, "z")
    a_all = [a_z, shifted(a_z, "x", shifts[1])]
    a_all += [shifted(a_z, "x", k) for k in shifts[2:]]
    b_all = exchanged(b_x, "z")
    a_other = [swapped(v) for v in a_all]
    b_other = swapped(b_all)
    origin = [lax.rem(x + (n_x - k), n_x) for k in shifts]
    wide = a.shape[2]
    shape = (n_x, n_z, n_c, own_rows, width)

    def spots(*pairs):
        return jnp.stack([v for pair in pairs for v in pair])

    out = placed_rows(
        shape,
        spots(*((origin[j], c) for j in (0, 1) for c in (core, 1 - core))),
        [(v[j], None, 0) for j in (0, 1) for v in (a_all, a_other)],
    )
    for a_last, b_last, c in ((a_all, b_all, core), (a_other, b_other, 1 - core)):
        out = placed_rows(
            shape,
            spots(*((origin[j], c) for j in range(2, n_x)), *((o, c) for o in origin)),
            [(v, None, 0) for v in a_last[2:]] + [(b_last, 1, wide)],
            out,
        )
    return out.reshape(n_x * n_z * n_c * own_rows, width)


def on_device(grads, skipped, master, moment_one, moment_two, bounds, step):
    flat_grads = grads[0, 0]
    rows_all, width = flat_grads.shape
    own_rows = master.shape[1]
    layers = bounds.shape[1] - 1
    n_section = lax.axis_size("section")
    n_all = lax.axis_size(ALL)
    summed = reduced_rows(flat_grads, own_rows)

    row_index = lax.axis_index(DP) * own_rows + jnp.arange(own_rows, dtype=jnp.int32)
    inside = (row_index[:, None] >= bounds[0, None, :-1]) & (
        row_index[:, None] < bounds[0, None, 1:]
    )
    row_squares = jnp.sum(summed * summed, axis=1)
    layer_part = jnp.sum(row_squares[:, None] * inside.astype(jnp.float32), axis=0)
    good = (MICRO - skipped).astype(jnp.float32)
    report = jnp.concatenate([layer_part, good])
    reports = exchanged(jnp.broadcast_to(report, (n_all, 1, layers + 1)), ALL)
    step_value = step[0].astype(jnp.float32)
    fix_one = 1.0 - jnp.power(beta_one, step_value)
    fix_two = 1.0 - jnp.power(beta_two, step_value)
    state = (moment_one[0], moment_two[0], master[0])
    sizes = (
        n_section,
        lax.axis_size("z"),
        width * GATHER_SHARE // 16,
        n_section * rows_all * width,
    )
    a, b, facts = normed_rows(
        reports,
        summed,
        *state,
        lax.axis_index("section").reshape(1),
        jnp.stack([fix_one, fix_two]),
        sizes,
    )
    gathered = gathered_rows(a, b)
    good, clip, grad_rms = facts[1, 0], facts[2, 0], facts[3, 0]
    layer_rows = (bounds[0, 1:] - bounds[0, :-1]).astype(jnp.float32)
    layer_norms = jnp.sqrt(facts[0, :layers] / (layer_rows * width))
    master_next, first_next, second_next = stepped(
        summed, good, clip, *state, fix_one, fix_two
    )
    return (
        gathered[None],
        master_next[None],
        first_next[None],
        second_next[None],
        layer_norms[None],
        grad_rms.reshape(1),
    )


def solution(mesh):
    split = Mesh(
        mesh.devices.reshape(mesh.shape["section"], 4, 8, 2), ("section", "x", "z", "c")
    )
    placed = (
        P("section", DP, None, None),
        P(DP),
        P("section", DP, None),
        P("section", DP, None),
        P("section", DP, None),
        P("section", None),
        P(),
    )

    return jax.shard_map(
        on_device,
        mesh=split,
        in_specs=placed,
        out_specs=(
            P("section", None, None),
            P("section", DP, None),
            P("section", DP, None),
            P("section", DP, None),
            P("section", None),
            P(),
        ),
        check_vma=False,
    )
```
